32 devices in a mesh: dp: 8 (over y, x, core), mp: 4 (over z).
Axes of the slice: x: 2, y: 2, z: 4, core: 2. Of those that a mesh axis runs over, the one named last changes fastest.
Arguments:
- vit_features: bfloat16 [32, 256, 1024], P('dp', 'mp'), may hold values from -6 to 6
- patch_counts: int32 [32], P('dp'), may hold values from 64 to 192
- text_counts: int32 [32], P('dp'), may hold values from 1 to 63
- tile_dest: int32 [32], P('dp'), may hold values from 0 to 7, as said below
- text_embeds: bfloat16 [32, 256, 4096], P('dp', 'mp'), may hold values from -6 to 6
- w_proj: bfloat16 [1024, 4096], replicated, may hold values from -0.1875 to 0.1875
- b_proj: float32 [4096], replicated, may hold values from -3 to 3
- norm_gain: float32 [1, 4096], replicated, may hold values from 0.1 to 1.9
- w_qkv: bfloat16 [1, 4096, 8, 512], P(None, 'dp', 'mp'), may hold values from -0.375 to 0.375
- w_out: bfloat16 [1, 8, 256, 4096], P(None, 'mp', None, 'dp'), may hold values from -0.125 to 0.125
Outputs:
- hidden_out: bfloat16 [32, 256, 4096], P('dp', 'mp')
The draws below stay inside these ranges and needn't reach their ends.
Inputs may be any that keep to these rules, and one draw needn't show every extreme that they name: `tile_dest`: each language-model rank receives exactly 4 tiles; one source rank sends at most 2 tiles to one language-model rank, and every source rank sends 2 to some rank.
All inputs are finite; a program needn't handle non-finite values.
Results may differ from the reference program's by a relative error of at most 0.01.
Values may be sent and summed in bfloat16 or wider, within the bound.
A program may use at most 128 MiB of HBM per device.

```python
import math
import jax
import jax.numpy as jnp
from jax import lax

D = 4096
VD = 1024
HS = 128
KVH = 8
GROUP = 2
LAYERS = 1
TILE = 256
IMG_DEV = 4
IMAGES = 32
N_DP = 8
N_MP = 4


def draw_tile_dest(key, part):
    rank_total = IMAGES // IMG_DEV
    owner_key = jax.random.fold_in(key, 101)
    shift_key = jax.random.fold_in(key, 202)
    order_key = jax.random.fold_in(key, 303)
    owners = jax.random.permutation(owner_key, rank_total).astype(jnp.int32)
    offsets = (1 + jax.random.permutation(shift_key, rank_total - 1)).astype(jnp.int32)
    shifts = jnp.concatenate([jnp.zeros((1,), jnp.int32), offsets[:IMG_DEV - 2], jnp.zeros((1,), jnp.int32)])
    scores = jax.random.randint(order_key, (rank_total, IMG_DEV), 0, 1 << 20) * IMG_DEV + jnp.arange(IMG_DEV, dtype=jnp.int32)[None, :]
    layers = jnp.argsort(scores, axis=1)
    picked = jnp.take(shifts, layers)
    sources = jnp.arange(rank_total, dtype=jnp.int32)[:, None]
    destinations = jnp.take(owners, (sources + picked) % rank_total)
    return destinations.reshape(IMAGES).astype(jnp.int32)


def draw_w_qkv(key, part):
    base_key = jax.random.fold_in(key, 404)
    width_all = (GROUP + 2) * HS
    base = jax.random.truncated_normal(base_key, -4.0, 4.0, (LAYERS, D, KVH, width_all), jnp.float32) * D ** (-0.5)
    return base.astype(jnp.bfloat16)


def set_ends(result, own_key, smallest, largest):
    spot = [jax.random.randint(jax.random.fold_in(own_key, axis), (), 0, length) for axis, length in enumerate(result.shape)]
    longest = result.shape.index(max(result.shape))
    neighbour = spot[:longest] + [(spot[longest] + 1) % result.shape[longest]] + spot[longest + 1:]
    return result.at[tuple(spot)].set(smallest).at[tuple(neighbour)].set(largest)


def levels(rng, shape, cuts, smallest, top_value):
    factor_of, own = 1.0, jax.random.fold_in(rng, 6)
    for axis_at, parts in cuts:
        draws = jnp.exp(jax.random.uniform(jax.random.fold_in(own, axis_at), (parts,), jnp.float32, smallest / len(cuts), top_value / len(cuts)))
        factor_of = factor_of * jnp.repeat(draws, shape[axis_at] // parts).reshape([-1 if axis == axis_at else 1 for axis in range(len(shape))])
    return factor_of


def noise(rng, extent, width, bound, cuts=(), kind=jnp.bfloat16):
    array = jax.random.normal(rng, extent, jnp.float32) * width
    if len(cuts) > 0:
        array = levels(rng, extent, cuts, -0.22, 0.18) * array
    return jnp.clip(array, min=-bound, max=bound).astype(kind)


def setup_inputs(seed: int = 0) -> dict:
    keys = jax.random.split(jax.random.key(seed), 11)
    return {
        "vit_features": noise(keys[0], (IMAGES, TILE, VD), 1.0, 6.0, ((0, 8), (1, 4))),
        "patch_counts": set_ends(jax.random.randint(keys[1], (IMAGES,), TILE // 4, 3 * TILE // 4 + 1), jax.random.fold_in(keys[1], 1), TILE // 4, (3 * TILE // 4 + 1) - 1).astype(jnp.int32),
        "text_counts": set_ends(jax.random.randint(keys[2], (IMAGES,), 1, TILE // 4), jax.random.fold_in(keys[2], 1), 1, (TILE // 4) - 1).astype(jnp.int32),
        "tile_dest": draw_tile_dest(jax.random.fold_in(keys[10], 71), 0),
        "text_embeds": noise(keys[4], (IMAGES, TILE, D), 1.0, 6.0, ((0, 8), (1, 4))),
        "w_proj": noise(keys[5], (VD, D), VD ** -0.5, 0.1875),
        "b_proj": noise(keys[6], (D,), 0.5, 3.0, (), jnp.float32),
        "norm_gain": jnp.clip(1.0 + 0.18 * jax.random.normal(keys[7], (LAYERS, D), jnp.float32), 0.1, 1.9),
        "w_qkv": draw_w_qkv(jax.random.fold_in(keys[10], 71), 0),
        "w_out": noise(keys[9], (LAYERS, KVH, GROUP * HS, D), (KVH * GROUP * HS) ** -0.5, 0.125, ((1, 4), (3, 8))),
    }


rope_base = 500000.0
epsilon = 1e-05

def tile_angles(tile_size, head_size):
    half_size = head_size // 2
    inverse = jnp.exp(-(2.0 * jnp.arange(half_size, dtype=jnp.float32) / head_size) * math.log(rope_base))
    positions = jnp.arange(tile_size, dtype=jnp.float32)
    return positions[:, None] * inverse[None, :]

def rotate_half(values, angles):
    half_size = values.shape[-1] // 2
    cosine = jnp.cos(angles)
    sine_part = jnp.sin(angles)
    first_half = values[..., :half_size]
    second = values[..., half_size:]
    return jnp.concatenate([first_half * cosine - second * sine_part, second * cosine + first_half * sine_part], axis=-1)

def attend_tile(operands):
    tile_queries, tile_keys, tile_values, length = operands
    score_scale = 1.0 / math.sqrt(HS)
    scores = jnp.einsum('rhge,che->hgrc', tile_queries.astype(jnp.float32), tile_keys.astype(jnp.float32)) * score_scale
    row_ids = jnp.arange(TILE, dtype=jnp.int32)[:, None]
    col_ids = jnp.arange(TILE, dtype=jnp.int32)[None, :]
    allowed = (col_ids <= row_ids) & (col_ids < length)
    scores = jnp.where(allowed, scores, -1e+30)
    row_max = lax.optimization_barrier(jnp.max(scores, axis=-1, keepdims=True))
    weights = jnp.where(allowed, jnp.exp(scores - row_max), 0.0)
    probabilities = (weights / lax.optimization_barrier(jnp.sum(weights, axis=-1, keepdims=True))).astype(jnp.bfloat16)
    return jnp.einsum('hgrc,che->rhge', probabilities.astype(jnp.float32), tile_values.astype(jnp.float32)).astype(jnp.bfloat16)

def decoder_attention(hidden, gain_row, weights_qkv, weights_out, lengths, angles):
    image_total = hidden.shape[0]
    as_float = hidden.astype(jnp.float32)
    mean_square = lax.optimization_barrier(jnp.mean(as_float * as_float, axis=-1, keepdims=True))
    normed = (as_float * lax.rsqrt(mean_square + epsilon) * gain_row).astype(jnp.bfloat16)
    joined_rows = jnp.dot(normed.reshape(image_total * TILE, D), weights_qkv.reshape(D, KVH * (GROUP + 2) * HS), preferred_element_type=jnp.float32)
    joined_rows = joined_rows.reshape(image_total, TILE, KVH, GROUP + 2, HS)
    queries = rotate_half(joined_rows[:, :, :, :GROUP, :], angles[None, :, None, None, :]).astype(jnp.bfloat16)
    key_heads = rotate_half(joined_rows[:, :, :, GROUP, :], angles[None, :, None, :]).astype(jnp.bfloat16)
    value_heads = joined_rows[:, :, :, GROUP + 1, :].astype(jnp.bfloat16)
    attended = lax.map(attend_tile, (queries, key_heads, value_heads, lengths))
    attended = attended.reshape(image_total * TILE, KVH * GROUP * HS)
    out_rows = weights_out.reshape(KVH * GROUP * HS, D)
    shard_width = KVH // N_MP * GROUP * HS
    summed = jnp.zeros((image_total * TILE, D), jnp.float32)
    for shard_idx in range(N_MP):
        partial_sum = jnp.dot(attended[:, shard_idx * shard_width:(shard_idx + 1) * shard_width], out_rows[shard_idx * shard_width:(shard_idx + 1) * shard_width], preferred_element_type=jnp.float32)
        summed = summed + lax.optimization_barrier(partial_sum.astype(jnp.bfloat16)).astype(jnp.float32)
    return (as_float + summed.reshape(image_total, TILE, D)).astype(jnp.bfloat16)

def reference(vit_features, patch_counts, text_counts, tile_dest, text_embeds, w_proj, b_proj, norm_gain, w_qkv, w_out):
    image_total = tile_dest.shape[0]
    dest_ids = jnp.arange(N_DP, dtype=jnp.int32)
    dest_hot = (tile_dest[:, None] == dest_ids[None, :]).astype(jnp.int32)
    earlier = jnp.cumsum(dest_hot, axis=0) - dest_hot
    slot_ids = lax.optimization_barrier(jnp.sum(earlier * dest_hot, axis=1)).astype(jnp.int32)
    targets = (tile_dest * IMG_DEV + slot_ids).astype(jnp.int32)
    sources = jnp.zeros((image_total,), jnp.int32).at[targets].set(jnp.arange(image_total, dtype=jnp.int32))
    placed = jnp.take(vit_features, sources, axis=0)
    projected = jnp.dot(placed.reshape(image_total * TILE, VD), w_proj, preferred_element_type=jnp.float32) + b_proj
    projected = projected.reshape(image_total, TILE, D)
    row_ids = jnp.arange(TILE, dtype=jnp.int32)[None, :, None]
    image_end = patch_counts[:, None, None]
    text_end = (patch_counts + text_counts)[:, None, None]
    hidden = jnp.where(row_ids < image_end, projected, jnp.where(row_ids < text_end, text_embeds.astype(jnp.float32), 0.0)).astype(jnp.bfloat16)
    lengths = patch_counts + text_counts
    angles = tile_angles(TILE, HS)
    for layer_idx in range(LAYERS):
        hidden = decoder_attention(hidden, norm_gain[layer_idx], w_qkv[layer_idx], w_out[layer_idx], lengths, angles)
    return hidden
```

```python
import functools
import math

import jax
import jax.numpy as jnp
from jax import lax
from jax.experimental import pallas as pl
from jax.experimental.pallas import tpu as pltpu
from jax.sharding import PartitionSpec as P

HS = 128
GROUP = 2
CAP = 2
LANES = 128
VMEM_BYTES = 60 * 1024 * 1024


rope_base = 500000.0
epsilon = 1e-05


def tile_angles(tile_size, head_size):
    half_size = head_size // 2
    inverse = jnp.exp(
        -(2.0 * jnp.arange(half_size, dtype=jnp.float32) / head_size) * math.log(rope_base)
    )
    positions = jnp.arange(tile_size, dtype=jnp.float32)
    return positions[:, None] * inverse[None, :]


def exchange_tiles(vit_features, tile_dest, rank_count):
    image_count, local_rows, vision_width = vit_features.shape
    dest_ids = jnp.arange(rank_count, dtype=jnp.int32)
    own_hot = (tile_dest[:, None] == dest_ids[None, :]).astype(jnp.int32)
    own_before = jnp.sum((jnp.cumsum(own_hot, axis=0) - own_hot) * own_hot, axis=1)
    targets = tile_dest * CAP + own_before
    placing = (targets[:, None] == jnp.arange(rank_count * CAP, dtype=jnp.int32)[None, :]).astype(
        jnp.bfloat16
    )
    flat_rows = vit_features.reshape(image_count, local_rows * vision_width)
    flat_rows = jnp.concatenate(
        [flat_rows, jnp.ones((image_count, LANES), flat_rows.dtype)], axis=1
    )
    outgoing = jnp.dot(placing.T, flat_rows, preferred_element_type=jnp.float32).astype(
        jnp.bfloat16
    )
    outgoing = outgoing.reshape(rank_count, CAP, -1)
    incoming = lax.all_to_all(outgoing, "dp", split_axis=0, concat_axis=0, tiled=True)
    incoming = incoming.reshape(rank_count * CAP, -1)
    filled = incoming[:, local_rows * vision_width].astype(jnp.int32)
    place = jnp.cumsum(filled) - filled
    selector = (
        (place[None, :] == jnp.arange(image_count, dtype=jnp.int32)[:, None]) & (filled[None, :] > 0)
    ).astype(jnp.bfloat16)
    arrived = jnp.dot(
        selector,
        incoming[:, : local_rows * vision_width],
        preferred_element_type=jnp.float32,
    )
    return arrived.astype(jnp.bfloat16).reshape(image_count, local_rows, vision_width)


def line_gather(block, axis_name, first_needed, last_needed):
    count = lax.axis_size(axis_name)
    by_offset = {0: block}
    passing = block
    for hop in range(1, count):
        pairs = [
            (i, i + 1)
            for i in range(hop - 1, count - 1)
            if first_needed <= i - hop + 1 <= last_needed
        ]
        if not pairs:
            break
        passing = lax.ppermute(passing, axis_name, pairs)
        by_offset[count - hop] = passing
    passing = block
    for hop in range(1, count):
        pairs = [
            (i, i - 1)
            for i in range(1, count - hop + 1)
            if first_needed <= i + hop - 1 <= last_needed
        ]
        if not pairs:
            break
        passing = lax.ppermute(passing, axis_name, pairs)
        by_offset[hop] = by_offset[hop] + passing if hop in by_offset else passing
    return by_offset


def doubling_gather(block, axis_name, split_axis, settle=None):
    count = lax.axis_size(axis_name)
    bits = count.bit_length() - 1
    outer = list(range(1, bits))
    orders = (outer, outer[1:] + outer[:1])

    def send(array, bit):
        return lax.ppermute(array, axis_name, [(i, i ^ (1 << bit)) for i in range(count)])

    def half_of(array, half):
        size = array.shape[split_axis] // 2
        return lax.slice_in_dim(array, half * size, (half + 1) * size, axis=split_axis)

    whole = {0: block}
    for bit in outer:
        whole[1 << bit] = send(block, bit)
    if settle is not None:
        whole = settle(whole)
    parts = ({}, {})
    for mask in range(2, count, 2):
        if mask in whole:
            continue
        for half in (0, 1):
            parts[half][mask] = None
    for half in (0, 1):
        reached = [0]
        for bit in orders[half]:
            for base in list(reached):
                mask = base | (1 << bit)
                reached.append(mask)
                if mask in whole:
                    continue
                origin = half_of(whole[base], half) if base in whole else parts[half][base]
                parts[half][mask] = send(origin, bit)
    pieces = [(mask, None, array) for mask, array in whole.items()]
    for half in (0, 1):
        pieces += [(mask, half, array) for mask, array in parts[half].items()]
    if bits > 0:
        pieces += [(mask | 1, half, send(array, 0)) for mask, half, array in pieces]
    return pieces


def attend_kernel(
    keys,
    local_rows,
    patch_ref,
    length_ref,
    images_ref,
    text_ref,
    proj_ref,
    bias_ref,
    gain_ref,
    cos_ref,
    sin_ref,
    *rest,
):
    pieces = rest[: len(keys)]
    attended_ref, own_ref, hidden_s, normed_s, joined_s = rest[len(keys) :]
    tile = pl.program_id(0)
    patches = patch_ref[tile]
    length = length_ref[tile]
    tile_size, model_width = hidden_s.shape
    window = text_ref.shape[1]
    image_rows = tile_size - window
    chunk = 512
    row_ids = lax.broadcasted_iota(jnp.int32, (tile_size, 1), 0)
    squares = jnp.zeros((tile_size, 1), jnp.float32)
    for start in range(0, model_width, chunk):
        columns = slice(start, start + chunk)
        projected = (
            jnp.dot(
                images_ref[0, :image_rows],
                proj_ref[:, columns],
                preferred_element_type=jnp.float32,
            )
            + bias_ref[:, columns]
        )
        text = text_ref[0, :, columns].astype(jnp.float32)
        texts = jnp.concatenate([text] * (tile_size // window), axis=0)
        texts = jnp.where(row_ids < length, texts, 0.0)
        top = jnp.where(row_ids[:image_rows] < patches, projected, texts[:image_rows])
        rows = jnp.concatenate([top, texts[image_rows:]], axis=0).astype(jnp.bfloat16)
        hidden_s[:, columns] = rows
        rows = rows.astype(jnp.float32)
        squares = squares + jnp.sum(rows * rows, axis=1, keepdims=True)
    factor = lax.rsqrt(squares / model_width + epsilon)
    for start in range(0, model_width, chunk):
        columns = slice(start, start + chunk)
        normed_s[:, columns] = (
            hidden_s[:, columns].astype(jnp.float32) * factor * gain_ref[:, columns]
        ).astype(jnp.bfloat16)
    own_start = pl.multiple_of(lax.axis_index("mp") * local_rows, local_rows)
    own_ref[0] = hidden_s[pl.ds(own_start, local_rows), :]

    rank = lax.axis_index("dp")
    width = joined_s.shape[1]
    half_width = width // 2
    for side in (0, 1):
        total = None
        for (mask, half), piece in zip(keys, pieces):
            if half is not None and half != side:
                continue
            depth = piece.shape[0]
            start = pl.multiple_of((rank ^ mask) * depth, depth)
            block = piece[...] if half is not None else piece[:, side * half_width : (side + 1) * half_width]
            term = jnp.dot(
                normed_s[:, pl.ds(start, depth)], block, preferred_element_type=jnp.float32
            )
            total = term if total is None else total + term
        joined_s[:, side * half_width : (side + 1) * half_width] = total

    cosine = cos_ref[...]
    sine = sin_ref[...]

    def rotated(start):
        values = joined_s[:, start : start + HS]
        return (values * cosine + pltpu.roll(values, HS // 2, 1) * sine).astype(jnp.bfloat16)

    col_ids = lax.broadcasted_iota(jnp.int32, (1, tile_size), 1)
    allowed = (col_ids <= row_ids) & (col_ids < length)
    head_width = (GROUP + 2) * HS
    outputs = []
    for first in range(0, width, head_width):
        head_keys = rotated(first + GROUP * HS)
        values = joined_s[:, first + (GROUP + 1) * HS : first + head_width].astype(jnp.bfloat16)
        for group in range(GROUP):
            queries = rotated(first + group * HS)
            scores = lax.dot_general(
                queries, head_keys, (((1,), (1,)), ((), ())), preferred_element_type=jnp.float32
            ) * (1.0 / math.sqrt(HS))
            scores = jnp.where(allowed, scores, -1e30)
            row_max = jnp.max(scores, axis=1, keepdims=True)
            weights = jnp.where(allowed, jnp.exp(scores - row_max), 0.0)
            weights = (weights / jnp.sum(weights, axis=1, keepdims=True)).astype(jnp.bfloat16)
            outputs.append(
                jnp.dot(weights, values, preferred_element_type=jnp.float32).astype(jnp.bfloat16)
            )
    attended = jnp.concatenate(outputs, axis=1)
    for part in range(tile_size // local_rows):
        attended_ref[part, 0] = attended[part * local_rows : (part + 1) * local_rows]


def output_kernel(keys, attended_ref, own_ref, *rest):
    count = len(keys)
    pieces = rest[:count]
    out_ref = rest[count]
    buffers = rest[count + 1 : 2 * count + 1]
    joined_s, sems = rest[2 * count + 1 :]
    copies = [
        pltpu.make_async_copy(piece, buffer, sems.at[index])
        for index, (piece, buffer) in enumerate(zip(pieces, buffers))
    ]
    for copy in copies:
        copy.start()
    parts, _, depth = attended_ref.shape
    for part in range(parts):
        joined_s[:, part * depth : (part + 1) * depth] = attended_ref[part]
    rank = lax.axis_index("dp")
    masks = {}
    for index, (mask, half) in enumerate(keys):
        masks.setdefault(mask, []).append((index, half))
    for mask, members in masks.items():
        width = pieces[members[0][0]].shape[1]
        columns = pl.ds(pl.multiple_of((rank ^ mask) * width, width), width)
        total = None
        for index, half in members:
            copies[index].wait()
            rows = buffers[index].shape[0]
            start = 0 if half is None else half * rows
            term = jnp.dot(
                joined_s[:, start : start + rows],
                buffers[index][...],
                preferred_element_type=jnp.float32,
            )
            total = term if total is None else total + term
        out_ref[:, columns] = (own_ref[:, columns].astype(jnp.float32) + total).astype(jnp.bfloat16)


def general_body(
    vit_features,
    patch_counts,
    text_counts,
    tile_dest,
    text_embeds,
    w_proj,
    b_proj,
    norm_gain,
    w_qkv,
    w_out,
):
    rank_count = lax.axis_size("dp")
    mp_count = lax.axis_size("mp")
    mp_rank = lax.axis_index("mp")
    image_count, local_rows, vision_width = vit_features.shape
    tile_size = local_rows * mp_count
    model_width = w_proj.shape[1]
    window = tile_size // 4
    lengths = patch_counts + text_counts

    own_rows = (mp_rank * local_rows + jnp.arange(local_rows, dtype=jnp.int32))[None, :, None]
    in_text = (own_rows >= patch_counts[:, None, None]) & (own_rows < lengths[:, None, None])
    text_rows = jnp.where(in_text, text_embeds, jnp.zeros_like(text_embeds))
    spans = window // local_rows
    if spans > 1:
        text_rows = jnp.concatenate(
            [
                jnp.where(mp_rank % spans == part, text_rows, jnp.zeros_like(text_rows))
                for part in range(spans)
            ],
            axis=1,
        )
    vit_features, text_rows = lax.optimization_barrier((vit_features, text_rows))
    text_rows = lax.psum(text_rows, "mp")

    out_depth = w_out.shape[1] * w_out.shape[2]
    out_width = w_out.shape[3]
    out_local = w_out.reshape(out_depth, out_width)
    out_blocks = line_gather(out_local, "mp", 0, mp_count - 1)
    out_columns = jnp.zeros((mp_count, out_depth, out_width), out_local.dtype)
    for offset, block in out_blocks.items():
        out_columns = lax.dynamic_update_index_in_dim(
            out_columns, block, (mp_rank + offset) % mp_count, 0
        )
    out_columns = out_columns.reshape(mp_count * out_depth, out_width)

    arrived = exchange_tiles(vit_features, tile_dest, rank_count)
    qkv_local = w_qkv.reshape(w_qkv.shape[1], -1)
    qkv_width = qkv_local.shape[1]
    qkv_pieces = doubling_gather(qkv_local, "dp", 1)
    qkv_keys = [(mask, half) for mask, half, _ in qkv_pieces]
    qkv_arrays = [array for _, _, array in qkv_pieces]

    def settle(whole):
        nonlocal text_rows, arrived, qkv_arrays
        text_rows, arrived, qkv_arrays, whole = lax.optimization_barrier(
            (text_rows, arrived, qkv_arrays, whole)
        )
        return whole

    out_pieces = doubling_gather(out_columns, "dp", 0, settle)
    images = lax.all_gather(arrived, "mp", axis=1, tiled=True)

    images, out_arrays = lax.optimization_barrier((images, [array for _, _, array in out_pieces]))

    angles = tile_angles(tile_size, HS)
    cosine, sine = jnp.cos(angles), jnp.sin(angles)
    cosine = jnp.concatenate([cosine, cosine], axis=1)
    sine = jnp.concatenate([-sine, sine], axis=1)

    def fixed(array):
        return pl.BlockSpec(array.shape, lambda i: (0,) * array.ndim)

    bias = b_proj.reshape(1, -1)
    gain = norm_gain.reshape(1, -1)
    attended, own_hidden = pl.pallas_call(
        functools.partial(attend_kernel, qkv_keys, local_rows),
        grid=(image_count,),
        in_specs=[
            pl.BlockSpec(memory_space=pltpu.SMEM),
            pl.BlockSpec(memory_space=pltpu.SMEM),
            pl.BlockSpec((1, tile_size, vision_width), lambda i: (i, 0, 0)),
            pl.BlockSpec((1, window, model_width), lambda i: (i, 0, 0)),
            fixed(w_proj),
            fixed(bias),
            fixed(gain),
            fixed(cosine),
            fixed(sine),
        ]
        + [fixed(array) for array in qkv_arrays],
        out_specs=[
            pl.BlockSpec((mp_count, 1, local_rows, out_depth), lambda i: (0, i, 0, 0)),
            pl.BlockSpec((1, local_rows, model_width), lambda i: (i, 0, 0)),
        ],
        out_shape=[
            jax.ShapeDtypeStruct((mp_count, image_count, local_rows, out_depth), jnp.bfloat16),
            jax.ShapeDtypeStruct((image_count, local_rows, model_width), jnp.bfloat16),
        ],
        scratch_shapes=[
            pltpu.VMEM((tile_size, model_width), jnp.bfloat16),
            pltpu.VMEM((tile_size, model_width), jnp.bfloat16),
            pltpu.VMEM((tile_size, qkv_width), jnp.float32),
        ],
        compiler_params=pltpu.CompilerParams(vmem_limit_bytes=VMEM_BYTES),
        cost_estimate=pl.CostEstimate(
            flops=2 * image_count * tile_size * model_width * (vision_width + qkv_width),
            bytes_accessed=2 * model_width * (vision_width + qkv_width),
            transcendentals=0,
        ),
        name="attend",
    )(
        patch_counts, lengths, images, text_rows, w_proj, bias, gain, cosine, sine, *qkv_arrays
    )

    attended = lax.all_to_all(attended, "mp", split_axis=0, concat_axis=0, tiled=True)

    rows = image_count * local_rows
    out_keys = [(mask, half) for mask, half, _ in out_pieces]
    vmem = pl.BlockSpec(memory_space=pltpu.VMEM)
    result = pl.pallas_call(
        functools.partial(output_kernel, out_keys),
        in_specs=[vmem, vmem] + [pl.BlockSpec(memory_space=pl.ANY)] * len(out_arrays),
        out_specs=vmem,
        out_shape=jax.ShapeDtypeStruct((rows, model_width), jnp.bfloat16),
        scratch_shapes=[pltpu.VMEM(array.shape, array.dtype) for array in out_arrays]
        + [
            pltpu.VMEM((rows, mp_count * out_depth), jnp.bfloat16),
            pltpu.SemaphoreType.DMA((len(out_arrays),)),
        ],
        compiler_params=pltpu.CompilerParams(vmem_limit_bytes=VMEM_BYTES),
        cost_estimate=pl.CostEstimate(
            flops=2 * rows * model_width * mp_count * out_depth,
            bytes_accessed=2 * model_width * mp_count * out_depth,
            transcendentals=0,
        ),
        name="output",
    )(
        attended.reshape(mp_count, rows, out_depth),
        own_hidden.reshape(rows, model_width),
        *out_arrays,
    )
    return result.reshape(image_count, local_rows, model_width)


def flipped(rank, mask):
    other = rank
    for bit in range(mask.bit_length()):
        if (mask >> bit) & 1:
            other = other + (1 - 2 * ((rank // (1 << bit)) % 2)) * (1 << bit)
    return other


def looked_up(index, table):
    value = table[0] * (1 - jnp.minimum(jnp.abs(index), 1))
    for at in range(1, len(table)):
        value = value + table[at] * (1 - jnp.minimum(jnp.abs(index - at), 1))
    return value


PLANE_STEPS = 10


class PlaneGather:
    def __init__(self, source, place, half_rows, send_sems, recv_sems, base):
        self.source, self.place, self.half_rows = source, place, half_rows
        self.send_sems, self.recv_sems, self.base = send_sems, recv_sems, base
        self.rank = lax.axis_index("dp")

    def part(self, ref, half):
        if half is None:
            return ref
        return ref.at[pl.ds(half * self.half_rows, self.half_rows)]

    def copy(self, index):
        mask, half, bit_mask, own = (
            (0, 0, 2, True),
            (0, 1, 2, True),
            (0, 0, 4, True),
            (0, 1, 4, True),
            (2, 0, 4, False),
            (4, 1, 2, False),
            (0, None, 1, True),
            (2, None, 1, False),
            (4, None, 1, False),
            (6, None, 1, False),
        )[index]
        slot = self.part(self.place(flipped(self.rank, mask)), half)
        source = self.part(self.source, half) if own else slot
        return pltpu.make_async_remote_copy(
            src_ref=source,
            dst_ref=slot,
            send_sem=self.send_sems.at[self.base + index],
            recv_sem=self.recv_sems.at[self.base + index],
            device_id={"dp": flipped(self.rank, bit_mask)},
            device_id_type=pl.DeviceIdType.MESH,
        )

    def start(self):
        for index in (0, 3, 1, 2, 6):
            self.copy(index).start()

    def relay(self):
        self.copy(0).wait_recv()
        self.copy(4).start()
        self.copy(3).wait_recv()
        self.copy(5).start()

    def forward(self):
        self.copy(1).wait_recv()
        self.copy(7).start()
        self.copy(2).wait_recv()
        self.copy(8).start()

    def forward_far(self):
        self.copy(4).wait_recv()
        self.copy(5).wait_recv()
        self.copy(9).start()

    def finish(self):
        for index in (6, 7, 8, 9):
            self.copy(index).wait_recv()

    def drain(self):
        for index in range(PLANE_STEPS):
            self.copy(index).wait_send()


def fused_kernel(
    orders,
    patch_ref,
    length_ref,
    images_hbm,
    text_hbm,
    proj_hbm,
    qkv_hbm,
    wout_hbm,
    bias_ref,
    gain_ref,
    cos_ref,
    sin_ref,
    out_hbm,
    imgs_s,
    imgz_s,
    text_s,
    qkv_s,
    wout_s,
    proj_s,
    hidden_s,
    normed_s,
    joined_s,
    leaving_s,
    joining_s,
    own_s,
    local_sems,
    img_send,
    img_recv,
    qkv_send,
    qkv_recv,
    wout_send,
    wout_recv,
    text_send,
    text_recv,
    imgz_send,
    imgz_recv,
    woutz_send,
    woutz_recv,
    att_send,
    att_recv,
    out_sems,
):
    rank = lax.axis_index("dp")
    z = lax.axis_index("mp")
    mp_count = joining_s.shape[0]
    last = mp_count - 1
    shards, tiles, local_rows, vision_width = imgz_s.shape
    ranks = imgs_s.shape[0]
    image_rows = tiles * local_rows
    tile_size, model_width = hidden_s.shape
    depth = qkv_hbm.shape[0]
    out_width = wout_hbm.shape[1]
    first = tile_size // 4 // local_rows
    chunk = 512

    def right(source, target, send_sem, recv_sem):
        return pltpu.make_async_remote_copy(
            src_ref=source,
            dst_ref=target,
            send_sem=send_sem,
            recv_sem=recv_sem,
            device_id={"mp": jnp.minimum(z + 1, last)},
            device_id_type=pl.DeviceIdType.MESH,
        )

    def left(source, target, send_sem, recv_sem):
        return pltpu.make_async_remote_copy(
            src_ref=source,
            dst_ref=target,
            send_sem=send_sem,
            recv_sem=recv_sem,
            device_id={"mp": jnp.maximum(z - 1, 0)},
            device_id_type=pl.DeviceIdType.MESH,
        )

    loads = [
        pltpu.make_async_copy(text_hbm, text_s.at[1], local_sems.at[0]),
        pltpu.make_async_copy(images_hbm, imgs_s.at[rank], local_sems.at[1]),
        pltpu.make_async_copy(
            qkv_hbm, qkv_s.at[pl.ds(pl.multiple_of(rank * depth, depth), depth)], local_sems.at[2]
        ),
        pltpu.make_async_copy(wout_hbm, wout_s.at[z, rank], local_sems.at[3]),
        pltpu.make_async_copy(proj_hbm, proj_s, local_sems.at[4]),
    ]

    img = PlaneGather(
        images_hbm,
        lambda r: imgs_s.at[r],
        images_hbm.shape[0] // 2,
        img_send,
        img_recv,
        0,
    )
    qkv = PlaneGather(
        qkv_hbm,
        lambda r: qkv_s.at[pl.ds(pl.multiple_of(r * depth, depth), depth)],
        depth // 2,
        qkv_send,
        qkv_recv,
        0,
    )

    def block_of(k):
        picked = 0
        for zz in range(mp_count):
            here = 1 - jnp.minimum(jnp.abs(z - zz), 1)
            picked = picked + here * looked_up(k, orders[zz])
        return picked

    def wout(k):
        block = block_of(k)
        return PlaneGather(
            wout_s.at[block, rank],
            lambda r: wout_s.at[block, r],
            wout_hbm.shape[0] // 2,
            wout_send,
            wout_recv,
            k * PLANE_STEPS,
        )

    def text_right(tile, origin):
        source = text_hbm.at[tile] if origin else text_s.at[0, tile]
        return right(source, text_s.at[0, tile], text_send.at[tile], text_recv.at[tile])

    def text_left(tile, origin):
        source = text_hbm.at[tile] if origin else text_s.at[2, tile]
        return left(
            source, text_s.at[2, tile], text_send.at[tiles + tile], text_recv.at[tiles + tile]
        )

    def merge(slot, tile):
        own_rows = z * local_rows + lax.broadcasted_iota(jnp.int32, (local_rows, 1), 0)
        valid = (own_rows >= patch_ref[tile]) & (own_rows < length_ref[tile])
        for start in range(0, model_width, chunk):
            columns = slice(start, start + chunk)
            text_s[slot, tile, :, columns] = jnp.where(
                valid,
                text_s[1, tile, :, columns].astype(jnp.float32),
                text_s[slot, tile, :, columns].astype(jnp.float32),
            ).astype(jnp.bfloat16)

    def text_slot(turn):
        tile = turn - (z - first)

        @pl.when((z > first) & (z < last) & (tile >= 0) & (tile < tiles))
        def _():
            at = jnp.clip(tile, 0, tiles - 1)
            text_right(at, False).wait_recv()
            merge(0, at)
            text_right(at, False).start()

        other = turn - (last - z)

        @pl.when((z > 0) & (z < last) & (other >= 0) & (other < tiles))
        def _():
            at = jnp.clip(other, 0, tiles - 1)
            text_left(at, False).wait_recv()
            merge(2, at)
            text_left(at, False).start()

    def woutz_right(block):
        part = wout_s.at[block, rank]
        return right(part, part, woutz_send.at[block], woutz_recv.at[block])

    def woutz_left(block):
        part = wout_s.at[block, rank]
        return left(part, part, woutz_send.at[mp_count + block], woutz_recv.at[block])

    def woutz_own_right():
        part = wout_s.at[z, rank]
        return right(wout_hbm, part, woutz_send.at[z], woutz_recv.at[z])

    def woutz_own_left():
        part = wout_s.at[z, rank]
        return left(wout_hbm, part, woutz_send.at[mp_count + z], woutz_recv.at[z])

    def woutz_step(k):
        block = block_of(k)
        woutz_right(block).wait_recv()

        @pl.when((block < z) & (z < last))
        def _():
            woutz_right(block).start()

        @pl.when((block > z) & (z > 0))
        def _():
            woutz_left(block).start()

    def imgz_right(shard):
        part = imgz_s.at[shard]
        return right(part, part, imgz_send.at[shard], imgz_recv.at[shard])

    def imgz_left(shard):
        part = imgz_s.at[shard]
        return left(part, part, imgz_send.at[shards + shard], imgz_recv.at[shard])

    def imgz_forwards(shard):
        return ((shard < z) & (z < last)) | ((shard > z) & (z > 0))

    def imgz_relay(k):
        shard = block_of(k)

        @pl.when((shard < shards) & imgz_forwards(shard))
        def _():
            imgz_right(shard).wait_recv()

            @pl.when(shard < z)
            def _():
                imgz_right(shard).start()

            @pl.when(shard > z)
            def _():
                imgz_left(shard).start()

    def imgz_arrive(k):
        shard = block_of(k)

        @pl.when((shard < shards) & jnp.logical_not(imgz_forwards(shard)))
        def _():
            imgz_right(shard).wait_recv()

    def select_images():
        row_ids = lax.broadcasted_iota(jnp.int32, (image_rows, 1), 0)
        lane_ids = lax.broadcasted_iota(jnp.int32, (1, image_rows), 1) % local_rows
        before = jnp.zeros((1, 1), jnp.float32)
        total = jnp.zeros((image_rows, vision_width), jnp.float32)
        for source in range(ranks):
            dests = imgs_s[source, image_rows : image_rows + 1, :image_rows].astype(jnp.float32)
            earlier = imgs_s[source, image_rows + 1 : image_rows + 2, :image_rows].astype(jnp.float32)
            match = dests == rank.astype(jnp.float32)
            slots = (before + earlier).astype(jnp.int32)
            target = jnp.where(match, slots * local_rows + lane_ids, -1)
            chosen = jnp.where(row_ids == target, 1.0, 0.0).astype(jnp.bfloat16)
            total = total + jnp.dot(
                chosen, imgs_s[source, :image_rows, :], preferred_element_type=jnp.float32
            )
            count = jnp.sum(match.astype(jnp.float32), axis=1, keepdims=True)
            before = before + count * (1.0 / local_rows)
        picked = total.astype(jnp.bfloat16)
        for tile in range(tiles):
            imgz_s[z, tile] = picked[tile * local_rows : (tile + 1) * local_rows]

    def attend(tile):
        patches = patch_ref[tile]
        length = length_ref[tile]
        window = local_rows
        image_part = shards * local_rows
        row_ids = lax.broadcasted_iota(jnp.int32, (tile_size, 1), 0)
        images = jnp.concatenate([imgz_s[shard, tile] for shard in range(shards)], axis=0)
        squares = jnp.zeros((tile_size, 1), jnp.float32)
        sides = [jnp.clip(block - z, -1, 1) + 1 for block in range(mp_count)]
        for start in range(0, model_width, chunk):
            columns = slice(start, start + chunk)
            projected = (
                jnp.dot(images, proj_s[:, columns], preferred_element_type=jnp.float32)
                + bias_ref[:, columns]
            )
            texts = jnp.concatenate(
                [
                    text_s[sides[block], tile, :, columns].astype(jnp.float32)
                    for block in range(first, mp_count)
                ],
                axis=0,
            )
            texts = jnp.where(row_ids[first * window :] < length, texts, 0.0)
            overlap = image_part - first * window
            middle = jnp.where(
                row_ids[first * window : image_part] < patches,
                projected[first * window :],
                texts[:overlap],
            )
            rows = jnp.concatenate(
                [projected[: first * window], middle, texts[overlap:]], axis=0
            ).astype(jnp.bfloat16)
            hidden_s[:, columns] = rows
            rows = rows.astype(jnp.float32)
            squares = squares + jnp.sum(rows * rows, axis=1, keepdims=True)
        factor = lax.rsqrt(squares / model_width + epsilon)
        for start in range(0, model_width, chunk):
            columns = slice(start, start + chunk)
            normed_s[:, columns] = (
                hidden_s[:, columns].astype(jnp.float32) * factor * gain_ref[:, columns]
            ).astype(jnp.bfloat16)
        own_start = pl.multiple_of(z * local_rows, local_rows)
        own_s[tile] = hidden_s[pl.ds(own_start, local_rows), :]

        width = joined_s.shape[1]
        piece = width // 2
        for start in range(0, width, piece):
            joined_s[:, start : start + piece] = jnp.dot(
                normed_s[...], qkv_s[:, start : start + piece], preferred_element_type=jnp.float32
            )

        cosine = cos_ref[...]
        sine = sin_ref[...]

        def rotated(start):
            values = joined_s[:, start : start + HS]
            return (values * cosine + pltpu.roll(values, HS // 2, 1) * sine).astype(jnp.bfloat16)

        col_ids = lax.broadcasted_iota(jnp.int32, (1, tile_size), 1)
        allowed = (col_ids <= row_ids) & (col_ids < length)
        head_width = (GROUP + 2) * HS
        outputs = []
        for begin in range(0, width, head_width):
            head_keys = rotated(begin + GROUP * HS)
            values = joined_s[:, begin + (GROUP + 1) * HS : begin + head_width].astype(jnp.bfloat16)
            for group in range(GROUP):
                queries = rotated(begin + group * HS)
                scores = lax.dot_general(
                    queries,
                    head_keys,
                    (((1,), (1,)), ((), ())),
                    preferred_element_type=jnp.float32,
                ) * (1.0 / math.sqrt(HS))
                scores = jnp.where(allowed, scores, -1e30)
                row_max = jnp.max(scores, axis=1, keepdims=True)
                weights = jnp.where(allowed, jnp.exp(scores - row_max), 0.0)
                weights = (weights / jnp.sum(weights, axis=1, keepdims=True)).astype(jnp.bfloat16)
                outputs.append(
                    jnp.dot(weights, values, preferred_element_type=jnp.float32).astype(jnp.bfloat16)
                )
        attended = jnp.concatenate(outputs, axis=1)
        for part in range(mp_count):
            leaving_s[part, tile] = attended[part * local_rows : (part + 1) * local_rows]

    def att_copy(part, source, tile):
        return pltpu.make_async_remote_copy(
            src_ref=leaving_s.at[part, tile],
            dst_ref=joining_s.at[source, tile],
            send_sem=att_send.at[part * tiles + tile],
            recv_sem=att_recv.at[source * tiles + tile],
            device_id={"mp": part},
            device_id_type=pl.DeviceIdType.MESH,
        )

    def send_attended(tile):
        for part in range(mp_count):

            @pl.when(part != z)
            def _():
                att_copy(part, z, tile).start()

        joining_s[z, tile] = leaving_s[z, tile]

    for load in loads:
        load.start()
    img.start()

    @pl.when(z == first)
    def _():
        for tile in range(tiles):
            text_right(tile, True).start()

    @pl.when(z == last)
    def _():
        for tile in range(tiles):
            text_left(tile, True).start()

    @pl.when((z < last) & (z != first))
    def _():
        woutz_own_right().start()

    @pl.when((z > 0) & (z != last))
    def _():
        woutz_own_left().start()

    loads[0].wait()
    img.relay()
    qkv.start()
    text_slot(1)
    img.forward()
    img.forward_far()
    img.finish()
    loads[1].wait()

    @pl.when(z < shards)
    def _():
        select_images()

        @pl.when(z < last)
        def _():
            imgz_right(z).start()

        @pl.when(z > 0)
        def _():
            imgz_left(z).start()

    @pl.when(z == first)
    def _():
        woutz_own_right().start()

    @pl.when(z == last)
    def _():
        woutz_own_left().start()

    text_slot(2)
    qkv.relay()
    loads[3].wait()
    wout(0).start()
    text_slot(3)
    imgz_relay(1)
    qkv.forward()
    text_slot(4)
    imgz_relay(2)
    qkv.forward_far()
    text_slot(5)
    for turn in range(6, tiles + mp_count - first - 1):
        text_slot(turn)
    wout(0).relay()
    imgz_relay(3)
    woutz_step(1)
    wout(1).start()
    wout(0).forward()
    qkv.finish()
    loads[2].wait()
    loads[4].wait()
    wout(1).relay()
    wout(0).forward_far()
    for k in range(1, mp_count):
        imgz_arrive(k)

    @pl.loop(0, tiles)
    def _(tile):
        @pl.when(z == 0)
        def _():
            text_left(tile, False).wait_recv()

        @pl.when(z == last)
        def _():
            text_right(tile, False).wait_recv()

        attend(tile)
        send_attended(tile)

        @pl.when(tile == 0)
        def _():
            woutz_step(2)
            wout(2).start()
            wout(1).forward()

        @pl.when(tile == 1)
        def _():
            wout(2).relay()
            wout(1).forward_far()
            woutz_step(3)
            wout(3).start()
            wout(2).forward()

        @pl.when(tile == 2)
        def _():
            wout(3).relay()
            wout(2).forward_far()

    wout(3).forward()
    wout(3).forward_far()
    for k in range(mp_count):
        wout(k).finish()
    for source in range(mp_count):

        @pl.when(source != z)
        def _():
            for tile in range(tiles):
                att_copy(z, source, tile).wait_recv()

    @pl.loop(0, ranks)
    def _(source):
        columns = pl.ds(pl.multiple_of(source * out_width, out_width), out_width)
        total = own_s[:, :, columns].reshape(image_rows, out_width).astype(jnp.float32)
        summed = None
        for block in range(mp_count):
            term = jnp.dot(
                joining_s[block].reshape(image_rows, -1),
                wout_s[block, source],
                preferred_element_type=jnp.float32,
            )
            summed = term if summed is None else summed + term
        own_s[:, :, columns] = (
            (total + summed).astype(jnp.bfloat16).reshape(tiles, local_rows, out_width)
        )
        pltpu.make_async_copy(
            own_s.at[:, :, columns], out_hbm.at[:, :, columns], out_sems.at[source]
        ).start()

    img.drain()
    qkv.drain()
    for k in range(mp_count):
        wout(k).drain()
    for tile in range(tiles):

        @pl.when((z >= first) & (z < last))
        def _():
            text_right(tile, False).wait_send()

        @pl.when(z > 0)
        def _():
            text_left(tile, False).wait_send()

        for part in range(mp_count):

            @pl.when(part != z)
            def _():
                att_copy(part, z, tile).wait_send()

    for block in range(mp_count):

        @pl.when((block <= z) & (z < last))
        def _():
            woutz_right(block).wait_send()

        @pl.when((block >= z) & (z > 0))
        def _():
            woutz_left(block).wait_send()

    for shard in range(shards):

        @pl.when((shard <= z) & (z < last))
        def _():
            imgz_right(shard).wait_send()

        @pl.when((shard >= z) & (z > 0))
        def _():
            imgz_left(shard).wait_send()

    @pl.loop(0, ranks)
    def _(source):
        columns = pl.ds(pl.multiple_of(source * out_width, out_width), out_width)
        pltpu.make_async_copy(
            own_s.at[:, :, columns], out_hbm.at[:, :, columns], out_sems.at[source]
        ).wait()


def fused_body(
    vit_features,
    patch_counts,
    text_counts,
    tile_dest,
    text_embeds,
    w_proj,
    b_proj,
    norm_gain,
    w_qkv,
    w_out,
):
    ranks = lax.axis_size("dp")
    mp_count = lax.axis_size("mp")
    tiles, local_rows, vision_width = vit_features.shape
    tile_size = local_rows * mp_count
    model_width = w_proj.shape[1]
    image_rows = tiles * local_rows
    shards = 3 * tile_size // 4 // local_rows
    lengths = patch_counts + text_counts

    earlier = [jnp.zeros((), jnp.int32)]
    for image in range(1, tiles):
        earlier.append(sum((tile_dest[image] == tile_dest[at]).astype(jnp.int32) for at in range(image)))
    header_rows = 32
    rows = lax.broadcasted_iota(jnp.int32, (header_rows, vision_width), 0)
    lanes = lax.broadcasted_iota(jnp.int32, (header_rows, vision_width), 1) // local_rows
    header = jnp.zeros((header_rows, vision_width), jnp.int32)
    for image in range(tiles):
        header = jnp.where(
            lanes == image, jnp.where(rows == 0, tile_dest[image], earlier[image]), header
        )
    images = jnp.concatenate(
        [vit_features.reshape(image_rows, vision_width), header.astype(jnp.bfloat16)], axis=0
    )
    qkv_local = w_qkv.reshape(w_qkv.shape[1], -1)
    depth, qkv_width = qkv_local.shape
    out_depth = w_out.shape[1] * w_out.shape[2]
    out_width = w_out.shape[3]
    out_local = w_out.reshape(out_depth, out_width)

    angles = tile_angles(tile_size, HS)
    cosine, sine = jnp.cos(angles), jnp.sin(angles)
    cosine = jnp.concatenate([cosine, cosine], axis=1)
    sine = jnp.concatenate([-sine, sine], axis=1)

    orders = []
    for here in range(mp_count):
        order = [here]
        for distance in range(1, mp_count):
            order += [at for at in (here - distance, here + distance) if 0 <= at < mp_count]
        orders.append(order)

    anywhere = pl.BlockSpec(memory_space=pl.ANY)
    smem = pl.BlockSpec(memory_space=pltpu.SMEM)
    vmem = pl.BlockSpec(memory_space=pltpu.VMEM)
    half = jnp.bfloat16
    dma = pltpu.SemaphoreType.DMA
    return pl.pallas_call(
        functools.partial(fused_kernel, orders),
        in_specs=[smem, smem] + [anywhere] * 5 + [vmem] * 4,
        out_specs=anywhere,
        out_shape=jax.ShapeDtypeStruct((tiles, local_rows, model_width), half),
        scratch_shapes=[
            pltpu.VMEM((ranks,) + images.shape, half),
            pltpu.VMEM((shards, tiles, local_rows, vision_width), half),
            pltpu.VMEM((3, tiles, local_rows, model_width), half),
            pltpu.VMEM((ranks * depth, qkv_width), half),
            pltpu.VMEM((mp_count, ranks, out_depth, out_width), half),
            pltpu.VMEM((vision_width, model_width), half),
            pltpu.VMEM((tile_size, model_width), half),
            pltpu.VMEM((tile_size, model_width), half),
            pltpu.VMEM((tile_size, qkv_width), jnp.float32),
            pltpu.VMEM((mp_count, tiles, local_rows, out_depth), half),
            pltpu.VMEM((mp_count, tiles, local_rows, out_depth), half),
            pltpu.VMEM((tiles, local_rows, model_width), half),
            dma((5,)),
            dma((PLANE_STEPS,)),
            dma((PLANE_STEPS,)),
            dma((PLANE_STEPS,)),
            dma((PLANE_STEPS,)),
            dma((mp_count * PLANE_STEPS,)),
            dma((mp_count * PLANE_STEPS,)),
            dma((2 * tiles,)),
            dma((2 * tiles,)),
            dma((2 * shards,)),
            dma((shards,)),
            dma((2 * mp_count,)),
            dma((mp_count,)),
            dma((mp_count * tiles,)),
            dma((mp_count * tiles,)),
            dma((ranks,)),
        ],
        compiler_params=pltpu.CompilerParams(
            vmem_limit_bytes=VMEM_BYTES, has_side_effects=True
        ),
        name="fused",
    )(
        patch_counts,
        lengths,
        images,
        text_embeds,
        w_proj,
        qkv_local,
        out_local,
        b_proj.reshape(1, -1),
        norm_gain.reshape(1, -1),
        cosine,
        sine,
    )


def body(*arrays):
    vit_features = arrays[0]
    local_rows = vit_features.shape[1]
    tile_size = local_rows * lax.axis_size("mp")
    outer_axes = (lax.axis_size("dp") // 2).bit_length() - 1
    if outer_axes == 2 and local_rows * 4 == tile_size:
        return fused_body(*arrays)
    return general_body(*arrays)


def solution(mesh):
    in_specs = (
        P("dp", "mp", None),
        P("dp"),
        P("dp"),
        P("dp"),
        P("dp", "mp", None),
        P(),
        P(),
        P(),
        P(None, "dp", "mp", None),
        P(None, "mp", None, "dp"),
    )
    out_specs = P("dp", "mp", None)
    return jax.shard_map(body, mesh=mesh, in_specs=in_specs, out_specs=out_specs, check_vma=False)
```

```python
import functools
import math

import jax
import jax.numpy as jnp
import numpy as np
from jax import lax
from jax.experimental import pallas as pl
from jax.experimental.pallas import tpu as pltpu
from jax.sharding import PartitionSpec as P

HS = 128
GROUP = 2
CAP = 2
LANES = 128
VMEM_BYTES = 60 * 1024 * 1024


rope_base = 500000.0
epsilon = 1e-05


def tile_angles(tile_size, head_size):
    half_size = head_size // 2
    inverse = jnp.exp(
        -(2.0 * jnp.arange(half_size, dtype=jnp.float32) / head_size) * math.log(rope_base)
    )
    positions = jnp.arange(tile_size, dtype=jnp.float32)
    return positions[:, None] * inverse[None, :]


def exchange_tiles(vit_features, tile_dest, rank_count):
    image_count, local_rows, vision_width = vit_features.shape
    dest_ids = jnp.arange(rank_count, dtype=jnp.int32)
    own_hot = (tile_dest[:, None] == dest_ids[None, :]).astype(jnp.int32)
    own_before = jnp.sum((jnp.cumsum(own_hot, axis=0) - own_hot) * own_hot, axis=1)
    targets = tile_dest * CAP + own_before
    placing = (targets[:, None] == jnp.arange(rank_count * CAP, dtype=jnp.int32)[None, :]).astype(
        jnp.bfloat16
    )
    flat_rows = vit_features.reshape(image_count, local_rows * vision_width)
    flat_rows = jnp.concatenate(
        [flat_rows, jnp.ones((image_count, LANES), flat_rows.dtype)], axis=1
    )
    outgoing = jnp.dot(placing.T, flat_rows, preferred_element_type=jnp.float32).astype(
        jnp.bfloat16
    )
    outgoing = outgoing.reshape(rank_count, CAP, -1)
    incoming = lax.all_to_all(outgoing, "dp", split_axis=0, concat_axis=0, tiled=True)
    incoming = incoming.reshape(rank_count * CAP, -1)
    filled = incoming[:, local_rows * vision_width].astype(jnp.int32)
    place = jnp.cumsum(filled) - filled
    selector = (
        (place[None, :] == jnp.arange(image_count, dtype=jnp.int32)[:, None]) & (filled[None, :] > 0)
    ).astype(jnp.bfloat16)
    arrived = jnp.dot(
        selector,
        incoming[:, : local_rows * vision_width],
        preferred_element_type=jnp.float32,
    )
    return arrived.astype(jnp.bfloat16).reshape(image_count, local_rows, vision_width)


def line_gather(block, axis_name, first_needed, last_needed):
    count = lax.axis_size(axis_name)
    by_offset = {0: block}
    passing = block
    for hop in range(1, count):
        pairs = [
            (i, i + 1)
            for i in range(hop - 1, count - 1)
            if first_needed <= i - hop + 1 <= last_needed
        ]
        if not pairs:
            break
        passing = lax.ppermute(passing, axis_name, pairs)
        by_offset[count - hop] = passing
    passing = block
    for hop in range(1, count):
        pairs = [
            (i, i - 1)
            for i in range(1, count - hop + 1)
            if first_needed <= i + hop - 1 <= last_needed
        ]
        if not pairs:
            break
        passing = lax.ppermute(passing, axis_name, pairs)
        by_offset[hop] = by_offset[hop] + passing if hop in by_offset else passing
    return by_offset


def doubling_gather(block, axis_name, split_axis, settle=None):
    count = lax.axis_size(axis_name)
    bits = count.bit_length() - 1
    outer = list(range(1, bits))
    orders = (outer, outer[1:] + outer[:1])

    def send(array, bit):
        return lax.ppermute(array, axis_name, [(i, i ^ (1 << bit)) for i in range(count)])

    def half_of(array, half):
        size = array.shape[split_axis] // 2
        return lax.slice_in_dim(array, half * size, (half + 1) * size, axis=split_axis)

    whole = {0: block}
    for bit in outer:
        whole[1 << bit] = send(block, bit)
    if settle is not None:
        whole = settle(whole)
    parts = ({}, {})
    for mask in range(2, count, 2):
        if mask in whole:
            continue
        for half in (0, 1):
            parts[half][mask] = None
    for half in (0, 1):
        reached = [0]
        for bit in orders[half]:
            for base in list(reached):
                mask = base | (1 << bit)
                reached.append(mask)
                if mask in whole:
                    continue
                origin = half_of(whole[base], half) if base in whole else parts[half][base]
                parts[half][mask] = send(origin, bit)
    pieces = [(mask, None, array) for mask, array in whole.items()]
    for half in (0, 1):
        pieces += [(mask, half, array) for mask, array in parts[half].items()]
    if bits > 0:
        pieces += [(mask | 1, half, send(array, 0)) for mask, half, array in pieces]
    return pieces


def attend_kernel(
    keys,
    local_rows,
    patch_ref,
    length_ref,
    images_ref,
    text_ref,
    proj_ref,
    bias_ref,
    gain_ref,
    cos_ref,
    sin_ref,
    *rest,
):
    pieces = rest[: len(keys)]
    attended_ref, own_ref, hidden_s, normed_s, joined_s = rest[len(keys) :]
    tile = pl.program_id(0)
    patches = patch_ref[tile]
    length = length_ref[tile]
    tile_size, model_width = hidden_s.shape
    window = text_ref.shape[1]
    image_rows = tile_size - window
    chunk = 512
    row_ids = lax.broadcasted_iota(jnp.int32, (tile_size, 1), 0)
    squares = jnp.zeros((tile_size, 1), jnp.float32)
    for start in range(0, model_width, chunk):
        columns = slice(start, start + chunk)
        projected = (
            jnp.dot(
                images_ref[0, :image_rows],
                proj_ref[:, columns],
                preferred_element_type=jnp.float32,
            )
            + bias_ref[:, columns]
        )
        text = text_ref[0, :, columns].astype(jnp.float32)
        texts = jnp.concatenate([text] * (tile_size // window), axis=0)
        texts = jnp.where(row_ids < length, texts, 0.0)
        top = jnp.where(row_ids[:image_rows] < patches, projected, texts[:image_rows])
        rows = jnp.concatenate([top, texts[image_rows:]], axis=0).astype(jnp.bfloat16)
        hidden_s[:, columns] = rows
        rows = rows.astype(jnp.float32)
        squares = squares + jnp.sum(rows * rows, axis=1, keepdims=True)
    factor = lax.rsqrt(squares / model_width + epsilon)
    for start in range(0, model_width, chunk):
        columns = slice(start, start + chunk)
        normed_s[:, columns] = (
            hidden_s[:, columns].astype(jnp.float32) * factor * gain_ref[:, columns]
        ).astype(jnp.bfloat16)
    own_start = pl.multiple_of(lax.axis_index("mp") * local_rows, local_rows)
    own_ref[0] = hidden_s[pl.ds(own_start, local_rows), :]

    rank = lax.axis_index("dp")
    width = joined_s.shape[1]
    half_width = width // 2
    for side in (0, 1):
        total = None
        for (mask, half), piece in zip(keys, pieces):
            if half is not None and half != side:
                continue
            depth = piece.shape[0]
            start = pl.multiple_of((rank ^ mask) * depth, depth)
            block = piece[...] if half is not None else piece[:, side * half_width : (side + 1) * half_width]
            term = jnp.dot(
                normed_s[:, pl.ds(start, depth)], block, preferred_element_type=jnp.float32
            )
            total = term if total is None else total + term
        joined_s[:, side * half_width : (side + 1) * half_width] = total

    cosine = cos_ref[...]
    sine = sin_ref[...]

    def rotated(start):
        values = joined_s[:, start : start + HS]
        return (values * cosine + pltpu.roll(values, HS // 2, 1) * sine).astype(jnp.bfloat16)

    col_ids = lax.broadcasted_iota(jnp.int32, (1, tile_size), 1)
    allowed = (col_ids <= row_ids) & (col_ids < length)
    head_width = (GROUP + 2) * HS
    outputs = []
    for first in range(0, width, head_width):
        head_keys = rotated(first + GROUP * HS)
        values = joined_s[:, first + (GROUP + 1) * HS : first + head_width].astype(jnp.bfloat16)
        for group in range(GROUP):
            queries = rotated(first + group * HS)
            scores = lax.dot_general(
                queries, head_keys, (((1,), (1,)), ((), ())), preferred_element_type=jnp.float32
            ) * (1.0 / math.sqrt(HS))
            scores = jnp.where(allowed, scores, -1e30)
            row_max = jnp.max(scores, axis=1, keepdims=True)
            weights = jnp.where(allowed, jnp.exp(scores - row_max), 0.0)
            weights = (weights / jnp.sum(weights, axis=1, keepdims=True)).astype(jnp.bfloat16)
            outputs.append(
                jnp.dot(weights, values, preferred_element_type=jnp.float32).astype(jnp.bfloat16)
            )
    attended = jnp.concatenate(outputs, axis=1)
    for part in range(tile_size // local_rows):
        attended_ref[part, 0] = attended[part * local_rows : (part + 1) * local_rows]


def output_kernel(keys, attended_ref, own_ref, *rest):
    count = len(keys)
    pieces = rest[:count]
    out_ref = rest[count]
    buffers = rest[count + 1 : 2 * count + 1]
    joined_s, sems = rest[2 * count + 1 :]
    copies = [
        pltpu.make_async_copy(piece, buffer, sems.at[index])
        for index, (piece, buffer) in enumerate(zip(pieces, buffers))
    ]
    for copy in copies:
        copy.start()
    parts, _, depth = attended_ref.shape
    for part in range(parts):
        joined_s[:, part * depth : (part + 1) * depth] = attended_ref[part]
    rank = lax.axis_index("dp")
    masks = {}
    for index, (mask, half) in enumerate(keys):
        masks.setdefault(mask, []).append((index, half))
    for mask, members in masks.items():
        width = pieces[members[0][0]].shape[1]
        columns = pl.ds(pl.multiple_of((rank ^ mask) * width, width), width)
        total = None
        for index, half in members:
            copies[index].wait()
            rows = buffers[index].shape[0]
            start = 0 if half is None else half * rows
            term = jnp.dot(
                joined_s[:, start : start + rows],
                buffers[index][...],
                preferred_element_type=jnp.float32,
            )
            total = term if total is None else total + term
        out_ref[:, columns] = (own_ref[:, columns].astype(jnp.float32) + total).astype(jnp.bfloat16)


def general_body(
    vit_features,
    patch_counts,
    text_counts,
    tile_dest,
    text_embeds,
    w_proj,
    b_proj,
    norm_gain,
    w_qkv,
    w_out,
):
    rank_count = lax.axis_size("dp")
    mp_count = lax.axis_size("mp")
    mp_rank = lax.axis_index("mp")
    image_count, local_rows, vision_width = vit_features.shape
    tile_size = local_rows * mp_count
    model_width = w_proj.shape[1]
    window = tile_size // 4
    lengths = patch_counts + text_counts

    own_rows = (mp_rank * local_rows + jnp.arange(local_rows, dtype=jnp.int32))[None, :, None]
    in_text = (own_rows >= patch_counts[:, None, None]) & (own_rows < lengths[:, None, None])
    text_rows = jnp.where(in_text, text_embeds, jnp.zeros_like(text_embeds))
    spans = window // local_rows
    if spans > 1:
        text_rows = jnp.concatenate(
            [
                jnp.where(mp_rank % spans == part, text_rows, jnp.zeros_like(text_rows))
                for part in range(spans)
            ],
            axis=1,
        )
    vit_features, text_rows = lax.optimization_barrier((vit_features, text_rows))
    text_rows = lax.psum(text_rows, "mp")

    out_depth = w_out.shape[1] * w_out.shape[2]
    out_width = w_out.shape[3]
    out_local = w_out.reshape(out_depth, out_width)
    out_blocks = line_gather(out_local, "mp", 0, mp_count - 1)
    out_columns = jnp.zeros((mp_count, out_depth, out_width), out_local.dtype)
    for offset, block in out_blocks.items():
        out_columns = lax.dynamic_update_index_in_dim(
            out_columns, block, (mp_rank + offset) % mp_count, 0
        )
    out_columns = out_columns.reshape(mp_count * out_depth, out_width)

    arrived = exchange_tiles(vit_features, tile_dest, rank_count)
    qkv_local = w_qkv.reshape(w_qkv.shape[1], -1)
    qkv_width = qkv_local.shape[1]
    qkv_pieces = doubling_gather(qkv_local, "dp", 1)
    qkv_keys = [(mask, half) for mask, half, _ in qkv_pieces]
    qkv_arrays = [array for _, _, array in qkv_pieces]

    def settle(whole):
        nonlocal text_rows, arrived, qkv_arrays
        text_rows, arrived, qkv_arrays, whole = lax.optimization_barrier(
            (text_rows, arrived, qkv_arrays, whole)
        )
        return whole

    out_pieces = doubling_gather(out_columns, "dp", 0, settle)
    images = lax.all_gather(arrived, "mp", axis=1, tiled=True)

    images, out_arrays = lax.optimization_barrier((images, [array for _, _, array in out_pieces]))

    angles = tile_angles(tile_size, HS)
    cosine, sine = jnp.cos(angles), jnp.sin(angles)
    cosine = jnp.concatenate([cosine, cosine], axis=1)
    sine = jnp.concatenate([-sine, sine], axis=1)

    def fixed(array):
        return pl.BlockSpec(array.shape, lambda i: (0,) * array.ndim)

    bias = b_proj.reshape(1, -1)
    gain = norm_gain.reshape(1, -1)
    attended, own_hidden = pl.pallas_call(
        functools.partial(attend_kernel, qkv_keys, local_rows),
        grid=(image_count,),
        in_specs=[
            pl.BlockSpec(memory_space=pltpu.SMEM),
            pl.BlockSpec(memory_space=pltpu.SMEM),
            pl.BlockSpec((1, tile_size, vision_width), lambda i: (i, 0, 0)),
            pl.BlockSpec((1, window, model_width), lambda i: (i, 0, 0)),
            fixed(w_proj),
            fixed(bias),
            fixed(gain),
            fixed(cosine),
            fixed(sine),
        ]
        + [fixed(array) for array in qkv_arrays],
        out_specs=[
            pl.BlockSpec((mp_count, 1, local_rows, out_depth), lambda i: (0, i, 0, 0)),
            pl.BlockSpec((1, local_rows, model_width), lambda i: (i, 0, 0)),
        ],
        out_shape=[
            jax.ShapeDtypeStruct((mp_count, image_count, local_rows, out_depth), jnp.bfloat16),
            jax.ShapeDtypeStruct((image_count, local_rows, model_width), jnp.bfloat16),
        ],
        scratch_shapes=[
            pltpu.VMEM((tile_size, model_width), jnp.bfloat16),
            pltpu.VMEM((tile_size, model_width), jnp.bfloat16),
            pltpu.VMEM((tile_size, qkv_width), jnp.float32),
        ],
        compiler_params=pltpu.CompilerParams(vmem_limit_bytes=VMEM_BYTES),
        cost_estimate=pl.CostEstimate(
            flops=2 * image_count * tile_size * model_width * (vision_width + qkv_width),
            bytes_accessed=2 * model_width * (vision_width + qkv_width),
            transcendentals=0,
        ),
        name="attend",
    )(
        patch_counts, lengths, images, text_rows, w_proj, bias, gain, cosine, sine, *qkv_arrays
    )

    attended = lax.all_to_all(attended, "mp", split_axis=0, concat_axis=0, tiled=True)

    rows = image_count * local_rows
    out_keys = [(mask, half) for mask, half, _ in out_pieces]
    vmem = pl.BlockSpec(memory_space=pltpu.VMEM)
    result = pl.pallas_call(
        functools.partial(output_kernel, out_keys),
        in_specs=[vmem, vmem] + [pl.BlockSpec(memory_space=pl.ANY)] * len(out_arrays),
        out_specs=vmem,
        out_shape=jax.ShapeDtypeStruct((rows, model_width), jnp.bfloat16),
        scratch_shapes=[pltpu.VMEM(array.shape, array.dtype) for array in out_arrays]
        + [
            pltpu.VMEM((rows, mp_count * out_depth), jnp.bfloat16),
            pltpu.SemaphoreType.DMA((len(out_arrays),)),
        ],
        compiler_params=pltpu.CompilerParams(vmem_limit_bytes=VMEM_BYTES),
        cost_estimate=pl.CostEstimate(
            flops=2 * rows * model_width * mp_count * out_depth,
            bytes_accessed=2 * model_width * mp_count * out_depth,
            transcendentals=0,
        ),
        name="output",
    )(
        attended.reshape(mp_count, rows, out_depth),
        own_hidden.reshape(rows, model_width),
        *out_arrays,
    )
    return result.reshape(image_count, local_rows, model_width)


def flipped(rank, mask):
    other = rank
    for bit in range(mask.bit_length()):
        if (mask >> bit) & 1:
            other = other + (1 - 2 * ((rank // (1 << bit)) % 2)) * (1 << bit)
    return other


def looked_up(index, table):
    value = table[0] * (1 - jnp.minimum(jnp.abs(index), 1))
    for at in range(1, len(table)):
        value = value + table[at] * (1 - jnp.minimum(jnp.abs(index - at), 1))
    return value


PLANE_STEPS = 10


class PlaneGather:
    def __init__(self, source, place, half_rows, send_sems, recv_sems, base):
        self.source, self.place, self.half_rows = source, place, half_rows
        self.send_sems, self.recv_sems, self.base = send_sems, recv_sems, base
        self.rank = lax.axis_index("dp")

    def part(self, ref, half):
        if half is None:
            return ref
        return ref.at[pl.ds(half * self.half_rows, self.half_rows)]

    def copy(self, index):
        mask, half, bit_mask, own = (
            (0, 0, 2, True),
            (0, 1, 2, True),
            (0, 0, 4, True),
            (0, 1, 4, True),
            (2, 0, 4, False),
            (4, 1, 2, False),
            (0, None, 1, True),
            (2, None, 1, False),
            (4, None, 1, False),
            (6, None, 1, False),
        )[index]
        slot = self.part(self.place(flipped(self.rank, mask)), half)
        source = self.part(self.source, half) if own else slot
        return pltpu.make_async_remote_copy(
            src_ref=source,
            dst_ref=slot,
            send_sem=self.send_sems.at[self.base + index],
            recv_sem=self.recv_sems.at[self.base + index],
            device_id={"dp": flipped(self.rank, bit_mask)},
            device_id_type=pl.DeviceIdType.MESH,
        )

    def start(self):
        for index in (0, 3, 1, 2, 6):
            self.copy(index).start()

    def relay(self):
        self.copy(0).wait_recv()
        self.copy(4).start()
        self.copy(3).wait_recv()
        self.copy(5).start()

    def forward(self):
        self.copy(1).wait_recv()
        self.copy(7).start()
        self.copy(2).wait_recv()
        self.copy(8).start()

    def forward_far(self):
        self.copy(4).wait_recv()
        self.copy(5).wait_recv()
        self.copy(9).start()

    def finish(self):
        for index in (6, 7, 8, 9):
            self.copy(index).wait_recv()

    def drain(self):
        for index in range(PLANE_STEPS):
            self.copy(index).wait_send()


(I_RELAY, I_FORWARD, I_FAR, I_FINISH, Q_START, Q_RELAY, Q_FORWARD, Q_FAR, Q_FINISH, W_START, W_RELAY, W_FORWARD,
 W_FAR, OWN, LOADS, TEXT_RIGHT, TEXT_LEFT, W_PASS, W_WAIT, SHARD_PASS, SHARD_WAIT, W_SEND, HELD, OUT) = range(24)
SET, ADD, END = range(3)

SCHEDULE = (
    (
        [
            (I_RELAY,), (Q_START,), (I_FORWARD,), (I_FAR,), (I_FINISH,), (OWN,),
            (Q_RELAY,), (LOADS, 3), (W_START, 0), (Q_FORWARD,), (Q_FAR,),
            (W_RELAY, 0), (W_WAIT, 1), (W_START, 1), (W_FORWARD, 0), (W_FAR, 0),
            (W_RELAY, 1), (W_WAIT, 2), (W_START, 2), (W_FORWARD, 1),
            (Q_FINISH,), (LOADS, 0, 2, 4, 5, 6, 7, 8), (SHARD_WAIT, 1), (SHARD_WAIT, 2),
        ],
        [
            (I_RELAY,), (Q_START,), (LOADS, 0), (I_FORWARD,), (W_PASS, 2), (I_FAR,),
            (I_FINISH,), (OWN,), (W_SEND,), (TEXT_LEFT, 0), (Q_RELAY,), (LOADS, 3), (W_START, 0),
            (SHARD_PASS, 0), (W_PASS, 0), (SHARD_PASS, 2), (Q_FORWARD,), (TEXT_LEFT, 1), (Q_FAR,),
            (W_RELAY, 0), (W_START, 1), (TEXT_LEFT, 2), (W_FORWARD, 0), (W_FAR, 0),
            (TEXT_LEFT, 3), (W_RELAY, 1), (W_START, 2), (Q_FINISH,), (LOADS, 2, 4, 5, 6, 7, 8),
        ],
        [
            (I_RELAY,), (Q_START,), (LOADS, 0), (TEXT_RIGHT, 0), (TEXT_LEFT, 0), (I_FORWARD,),
            (I_FAR,), (I_FINISH,), (OWN,), (TEXT_RIGHT, 1), (TEXT_LEFT, 1), (Q_RELAY,),
            (LOADS, 3), (W_START, 0), (TEXT_RIGHT, 2), (TEXT_LEFT, 2), (Q_FORWARD,), (TEXT_RIGHT, 3), (TEXT_LEFT, 3),
            (Q_FAR,), (SHARD_PASS, 1), (W_RELAY, 0), (W_PASS, 3), (W_START, 1), (W_FORWARD, 0),
            (W_PASS, 1), (W_FAR, 0), (W_RELAY, 1), (W_START, 2), (SHARD_PASS, 0),
            (W_FORWARD, 1), (Q_FINISH,), (LOADS, 2, 4, 5, 6, 7, 8),
        ],
        [
            (I_RELAY,), (Q_START,), (I_FORWARD,), (I_FAR,), (I_FINISH,), (OWN,),
            (Q_RELAY,), (LOADS, 3), (W_START, 0), (Q_FORWARD,), (Q_FAR,),
            (W_RELAY, 0), (W_WAIT, 2), (W_START, 1), (W_FORWARD, 0), (W_FAR, 0),
            (W_RELAY, 1), (W_FORWARD, 1), (W_FAR, 1), (W_WAIT, 1), (W_START, 2),
            (Q_FINISH,), (LOADS, 0, 2, 4, 5, 6, 7, 8), (SHARD_WAIT, 2), (SHARD_WAIT, 1), (W_RELAY, 2),
            (SHARD_WAIT, 0),
        ],
    ),
    ([], [], [], []),
    (
        [(W_FAR, 1)],
        [(W_FORWARD, 1), (W_PASS, 3)],
        [(W_FAR, 1)],
        [(W_FORWARD, 2)],
    ),
    (
        [(W_RELAY, 2)],
        [(W_FAR, 1)],
        [(W_PASS, 0), (W_RELAY, 2), (W_START, 3)],
        [(W_FAR, 2), (W_WAIT, 0), (W_START, 3)],
    ),
    (
        [(W_FORWARD, 2)],
        [(W_RELAY, 2), (W_START, 3)],
        [(W_FORWARD, 2)],
        [(W_RELAY, 3)],
    ),
    (
        [
            (W_FAR, 2), (OUT, 0, SET), (W_WAIT, 3), (W_START, 3), (OUT, 1, ADD), (HELD,),
            (W_RELAY, 3), (OUT, 2, ADD), (W_FORWARD, 3), (W_FAR, 3), (OUT, 3, END),
        ],
        [
            (W_FORWARD, 2), (OUT, 1, SET), (W_FAR, 2), (W_RELAY, 3),
            (OUT, 0, ADD), (W_FORWARD, 3), (OUT, 2, ADD), (HELD,), (W_FAR, 3),
            (OUT, 3, END),
        ],
        [
            (W_FAR, 2), (OUT, 2, SET), (W_RELAY, 3), (OUT, 1, ADD), (HELD,),
            (W_FORWARD, 3), (W_FAR, 3), (OUT, 0, ADD), (OUT, 3, END),
        ],
        [
            (OUT, 3, SET), (W_FORWARD, 3), (OUT, 2, ADD), (W_FAR, 3),
            (OUT, 1, ADD), (OUT, 0, END),
        ],
    ),
)


HELD_BACK = ((3,), (3,), (0, 3), ())


def fused_kernel(
    orders,
    patch_ref,
    text_count_ref,
    dest_ref,
    images_hbm,
    text_hbm,
    proj_hbm,
    qkv_hbm,
    wout_hbm,
    bias_hbm,
    gain_hbm,
    cos_hbm,
    sin_hbm,
    out_hbm,
    bias_ref,
    gain_ref,
    cos_ref,
    sin_ref,
    dests_s,
    imgs_s,
    imgz_s,
    text_s,
    qkv_s,
    wout_s,
    proj_s,
    hidden_s,
    normed_s,
    joined_s,
    leaving_s,
    joining_s,
    own_s,
    summed_s,
    local_sems,
    dest_send,
    dest_recv,
    img_send,
    img_recv,
    qkv_send,
    qkv_recv,
    wout_send,
    wout_recv,
    text_send,
    text_recv,
    imgz_send,
    imgz_recv,
    woutz_send,
    woutz_recv,
    att_send,
    att_recv,
    out_sems,
):
    rank = lax.axis_index("dp")
    z = lax.axis_index("mp")
    mp_count = joining_s.shape[0]
    last = mp_count - 1
    shards, tiles, local_rows, vision_width = imgz_s.shape
    ranks = imgs_s.shape[0]
    image_rows = tiles * local_rows
    tile_size, model_width = hidden_s.shape
    depth = qkv_hbm.shape[0]
    out_width = wout_hbm.shape[1]
    first = tile_size // 4 // local_rows
    chunk = 512

    def right(source, target, send_sem, recv_sem):
        return pltpu.make_async_remote_copy(
            src_ref=source,
            dst_ref=target,
            send_sem=send_sem,
            recv_sem=recv_sem,
            device_id={"mp": jnp.minimum(z + 1, last)},
            device_id_type=pl.DeviceIdType.MESH,
        )

    def left(source, target, send_sem, recv_sem):
        return pltpu.make_async_remote_copy(
            src_ref=source,
            dst_ref=target,
            send_sem=send_sem,
            recv_sem=recv_sem,
            device_id={"mp": jnp.maximum(z - 1, 0)},
            device_id_type=pl.DeviceIdType.MESH,
        )

    loads = [
        pltpu.make_async_copy(text_hbm, text_s.at[1], local_sems.at[0]),
        pltpu.make_async_copy(images_hbm, imgs_s.at[rank], local_sems.at[1]),
        pltpu.make_async_copy(
            qkv_hbm, qkv_s.at[pl.ds(pl.multiple_of(rank * depth, depth), depth)], local_sems.at[2]
        ),
        pltpu.make_async_copy(wout_hbm, wout_s.at[z, rank], local_sems.at[3]),
        pltpu.make_async_copy(proj_hbm, proj_s, local_sems.at[4]),
        pltpu.make_async_copy(cos_hbm, cos_ref, local_sems.at[5]),
        pltpu.make_async_copy(bias_hbm, bias_ref, local_sems.at[6]),
        pltpu.make_async_copy(gain_hbm, gain_ref, local_sems.at[7]),
        pltpu.make_async_copy(sin_hbm, sin_ref, local_sems.at[8]),
    ]

    img = PlaneGather(
        images_hbm,
        lambda r: imgs_s.at[r],
        images_hbm.shape[0] // 2,
        img_send,
        img_recv,
        0,
    )
    qkv = PlaneGather(
        qkv_hbm,
        lambda r: qkv_s.at[pl.ds(pl.multiple_of(r * depth, depth), depth)],
        depth // 2,
        qkv_send,
        qkv_recv,
        0,
    )

    def block_of(k):
        picked = 0
        for zz in range(mp_count):
            here = 1 - jnp.minimum(jnp.abs(z - zz), 1)
            picked = picked + here * looked_up(k, orders[zz])
        return picked

    def wout(k, here=None):
        block = block_of(k) if here is None else orders[here][k]
        return PlaneGather(
            wout_s.at[block, rank],
            lambda r: wout_s.at[block, r],
            wout_hbm.shape[0] // 2,
            wout_send,
            wout_recv,
            k * PLANE_STEPS,
        )

    def text_right(tile, origin):
        source = text_hbm.at[tile] if origin else text_s.at[0, tile]
        return right(source, text_s.at[0, tile], text_send.at[tile], text_recv.at[tile])

    def text_left(tile, origin):
        source = text_hbm.at[tile] if origin else text_s.at[2, tile]
        return left(
            source, text_s.at[2, tile], text_send.at[tiles + tile], text_recv.at[tiles + tile]
        )

    def merge(slot, tile):
        own_rows = z * local_rows + lax.broadcasted_iota(jnp.int32, (local_rows, 1), 0)
        length = patch_ref[tile] + text_count_ref[tile]
        valid = (own_rows >= patch_ref[tile]) & (own_rows < length)
        for start in range(0, model_width, chunk):
            columns = slice(start, start + chunk)
            text_s[slot, tile, :, columns] = jnp.where(
                valid,
                text_s[1, tile, :, columns].astype(jnp.float32),
                text_s[slot, tile, :, columns].astype(jnp.float32),
            ).astype(jnp.bfloat16)

    def pass_text_right(tile):
        text_right(tile, False).wait_recv()
        merge(0, tile)
        text_right(tile, False).start()

    def pass_text_left(tile):
        text_left(tile, False).wait_recv()
        merge(2, tile)
        text_left(tile, False).start()

    def woutz_right(block):
        part = wout_s.at[block, rank]
        return right(part, part, woutz_send.at[block], woutz_recv.at[block])

    def woutz_left(block):
        part = wout_s.at[block, rank]
        return left(part, part, woutz_send.at[mp_count + block], woutz_recv.at[block])

    def woutz_own_right():
        part = wout_s.at[z, rank]
        return right(wout_hbm, part, woutz_send.at[z], woutz_recv.at[z])

    def woutz_own_left():
        part = wout_s.at[z, rank]
        return left(wout_hbm, part, woutz_send.at[mp_count + z], woutz_recv.at[z])

    def wait_block(block):
        woutz_right(block).wait_recv()

    def pass_block(here, block):
        wait_block(block)
        (woutz_right(block) if block < here else woutz_left(block)).start()

    def imgz_right(shard):
        part = imgz_s.at[shard]
        return right(part, part, imgz_send.at[shard], imgz_recv.at[shard])

    def imgz_left(shard):
        part = imgz_s.at[shard]
        return left(part, part, imgz_send.at[shards + shard], imgz_recv.at[shard])

    def wait_shard(shard):
        imgz_right(shard).wait_recv()

    def pass_shard(here, shard):
        wait_shard(shard)
        (imgz_right(shard) if shard < here else imgz_left(shard)).start()

    def dest_copy(mask):
        return pltpu.make_async_remote_copy(
            src_ref=dests_s.at[rank],
            dst_ref=dests_s.at[rank],
            send_sem=dest_send.at[mask],
            recv_sem=dest_recv.at[mask],
            device_id={"dp": flipped(rank, mask)},
            device_id_type=pl.DeviceIdType.MESH,
        )

    def select_images():
        row_ids = lax.broadcasted_iota(jnp.int32, (image_rows, 1), 0)
        lanes = lax.broadcasted_iota(jnp.int32, (1, image_rows), 1)
        image_ids, lane_rows = lanes // local_rows, lanes % local_rows
        before = jnp.zeros((1, 1), jnp.int32)
        total = jnp.zeros((image_rows, vision_width), jnp.float32)
        for source in range(ranks):
            match = jnp.zeros((1, image_rows), jnp.bool_)
            slots = jnp.zeros((1, image_rows), jnp.int32)
            for image in range(tiles):
                mine = dests_s[source, image : image + 1, :1] == rank
                match = match | ((image_ids == image) & mine)
                slots = jnp.where(image_ids == image, before, slots)
                before = before + mine.astype(jnp.int32)
            target = jnp.where(match, slots * local_rows + lane_rows, -1)
            chosen = jnp.where(row_ids == target, 1.0, 0.0).astype(jnp.bfloat16)
            total = total + jnp.dot(chosen, imgs_s[source], preferred_element_type=jnp.float32)
        picked = total.astype(jnp.bfloat16)
        for tile in range(tiles):
            imgz_s[z, tile] = picked[tile * local_rows : (tile + 1) * local_rows]

    def attend(tile):
        patches = patch_ref[tile]
        length = patch_ref[tile] + text_count_ref[tile]
        window = local_rows
        image_part = shards * local_rows
        row_ids = lax.broadcasted_iota(jnp.int32, (tile_size, 1), 0)
        images = jnp.concatenate([imgz_s[shard, tile] for shard in range(shards)], axis=0)
        squares = jnp.zeros((tile_size, 1), jnp.float32)
        sides = [jnp.clip(block - z, -1, 1) + 1 for block in range(mp_count)]
        for start in range(0, model_width, chunk):
            columns = slice(start, start + chunk)
            projected = (
                jnp.dot(images, proj_s[:, columns], preferred_element_type=jnp.float32)
                + bias_ref[:, columns]
            )
            texts = jnp.concatenate(
                [
                    text_s[sides[block], tile, :, columns].astype(jnp.float32)
                    for block in range(first, mp_count)
                ],
                axis=0,
            )
            texts = jnp.where(row_ids[first * window :] < length, texts, 0.0)
            overlap = image_part - first * window
            middle = jnp.where(
                row_ids[first * window : image_part] < patches,
                projected[first * window :],
                texts[:overlap],
            )
            rows = jnp.concatenate(
                [projected[: first * window], middle, texts[overlap:]], axis=0
            ).astype(jnp.bfloat16)
            hidden_s[:, columns] = rows
            rows = rows.astype(jnp.float32)
            squares = squares + jnp.sum(rows * rows, axis=1, keepdims=True)
        factor = lax.rsqrt(squares / model_width + epsilon)
        for start in range(0, model_width, chunk):
            columns = slice(start, start + chunk)
            normed_s[:, columns] = (
                hidden_s[:, columns].astype(jnp.float32) * factor * gain_ref[:, columns]
            ).astype(jnp.bfloat16)
        own_start = pl.multiple_of(z * local_rows, local_rows)
        own_s[tile] = hidden_s[pl.ds(own_start, local_rows), :]

        width = joined_s.shape[1]
        piece = width // 2
        for start in range(0, width, piece):
            joined_s[:, start : start + piece] = jnp.dot(
                normed_s[...], qkv_s[:, start : start + piece], preferred_element_type=jnp.float32
            )

        cosine = cos_ref[...]
        sine = sin_ref[...]

        def rotated(start):
            values = joined_s[:, start : start + HS]
            return (values * cosine + pltpu.roll(values, HS // 2, 1) * sine).astype(jnp.bfloat16)

        col_ids = lax.broadcasted_iota(jnp.int32, (1, tile_size), 1)
        allowed = (col_ids <= row_ids) & (col_ids < length)
        head_width = (GROUP + 2) * HS
        outputs = []
        for begin in range(0, width, head_width):
            head_keys = rotated(begin + GROUP * HS)
            values = joined_s[:, begin + (GROUP + 1) * HS : begin + head_width].astype(jnp.bfloat16)
            for group in range(GROUP):
                queries = rotated(begin + group * HS)
                scores = lax.dot_general(
                    queries,
                    head_keys,
                    (((1,), (1,)), ((), ())),
                    preferred_element_type=jnp.float32,
                ) * (1.0 / math.sqrt(HS))
                scores = jnp.where(allowed, scores, -1e30)
                row_max = jnp.max(scores, axis=1, keepdims=True)
                weights = jnp.where(allowed, jnp.exp(scores - row_max), 0.0)
                weights = (weights / jnp.sum(weights, axis=1, keepdims=True)).astype(jnp.bfloat16)
                outputs.append(
                    jnp.dot(weights, values, preferred_element_type=jnp.float32).astype(jnp.bfloat16)
                )
        attended = jnp.concatenate(outputs, axis=1)
        for part in range(mp_count):
            leaving_s[part, tile] = attended[part * local_rows : (part + 1) * local_rows]

    def att_copy(part, source, tile):
        return pltpu.make_async_remote_copy(
            src_ref=leaving_s.at[part, tile],
            dst_ref=joining_s.at[source, tile],
            send_sem=att_send.at[part * tiles + tile],
            recv_sem=att_recv.at[source * tiles + tile],
            device_id={"mp": part},
            device_id_type=pl.DeviceIdType.MESH,
        )

    def send_attended(tile):
        for part in range(mp_count):
            senders = [at for at in range(mp_count) if at != part and part not in HELD_BACK[at]]
            for at in senders:

                @pl.when(z == at)
                def _():
                    att_copy(part, z, tile).start()

        joining_s[z, tile] = leaving_s[z, tile]

    def add_output(here, block, stage):
        wout(orders[here].index(block), here).finish()
        if block != here:
            for tile in range(tiles):
                att_copy(here, block, tile).wait_recv()

        @pl.loop(0, ranks)
        def _(source):
            columns = pl.ds(pl.multiple_of(source * out_width, out_width), out_width)
            term = jnp.dot(
                joining_s[block].reshape(image_rows, -1),
                wout_s[block, source],
                preferred_element_type=jnp.float32,
            )
            if stage == SET:
                hidden = own_s[:, :, columns].reshape(image_rows, out_width)
                summed_s[:, columns] = hidden.astype(jnp.float32) + term
            elif stage == ADD:
                summed_s[:, columns] = summed_s[:, columns] + term
            else:
                total = (summed_s[:, columns] + term).astype(jnp.bfloat16)
                own_s[:, :, columns] = total.reshape(tiles, local_rows, out_width)
                out_copy(source).start()

    def out_copy(source):
        columns = pl.ds(pl.multiple_of(source * out_width, out_width), out_width)
        return pltpu.make_async_copy(
            own_s.at[:, :, columns], out_hbm.at[:, :, columns], out_sems.at[source]
        )

    def first_sends(here):
        if here == first:
            for tile in range(tiles):
                text_right(tile, True).start()
        if here == last:
            for tile in range(tiles):
                text_left(tile, True).start()
        if here < last and here != first:
            woutz_own_right().start()
        if here > 0:
            woutz_own_left().start()

    def own_images(here):
        loads[1].wait()
        for mask in range(1, ranks):
            dest_copy(mask).wait_recv()
        if here < shards:
            select_images()
            if here > 0:
                imgz_left(here).start()
            if here < last:
                imgz_right(here).start()

    def run(here, steps):
        for step, *numbers in steps:
            if step == OWN:
                own_images(here)
            elif step == LOADS:
                for at in numbers:
                    loads[at].wait()
            elif step == HELD:
                for tile in range(tiles):
                    for part in HELD_BACK[here]:
                        att_copy(part, here, tile).start()
            elif step == W_SEND:
                woutz_own_right().start()
            elif step in (OUT, W_PASS, SHARD_PASS):
                {OUT: add_output, W_PASS: pass_block, SHARD_PASS: pass_shard}[step](here, *numbers)
            elif step in (W_START, W_RELAY, W_FORWARD, W_FAR):
                block = wout(numbers[0], here)
                {
                    W_START: block.start,
                    W_RELAY: block.relay,
                    W_FORWARD: block.forward,
                    W_FAR: block.forward_far,
                }[step]()
            else:
                {
                    I_RELAY: img.relay,
                    I_FORWARD: img.forward,
                    I_FAR: img.forward_far,
                    I_FINISH: img.finish,
                    Q_START: qkv.start,
                    Q_RELAY: qkv.relay,
                    Q_FORWARD: qkv.forward,
                    Q_FAR: qkv.forward_far,
                    Q_FINISH: qkv.finish,
                    TEXT_RIGHT: pass_text_right,
                    TEXT_LEFT: pass_text_left,
                    W_WAIT: wait_block,
                    SHARD_WAIT: wait_shard,
                }[step](*numbers)

    def at_each_place(plan):
        for here in range(mp_count):
            if plan[here]:

                @pl.when(z == here)
                def _(here=here):
                    run(here, plan[here])

    for at in (0, 1, 3):
        loads[at].start()
    for image in range(tiles):
        dests_s[rank, image : image + 1, :] = jnp.full((1, LANES), dest_ref[image], jnp.int32)
    barrier = pltpu.get_barrier_semaphore()
    for mask in range(1, ranks):
        pl.semaphore_signal(
            barrier,
            inc=1,
            device_id={"dp": flipped(rank, mask)},
            device_id_type=pl.DeviceIdType.MESH,
        )
    for part in range(mp_count):

        @pl.when(part != z)
        def _():
            pl.semaphore_signal(
                barrier,
                inc=1,
                device_id={"mp": part},
                device_id_type=pl.DeviceIdType.MESH,
            )

    pl.semaphore_wait(barrier, ranks - 1 + mp_count - 1)
    img.start()
    for here in range(mp_count):

        @pl.when(z == here)
        def _(here=here):
            first_sends(here)

    for mask in range(1, ranks):
        dest_copy(mask).start()
    for at in (2, 4, 5, 6, 7, 8):
        loads[at].start()
    at_each_place(SCHEDULE[0])

    @pl.loop(0, tiles)
    def _(tile):
        for at in range(len(SCHEDULE) - 2):

            @pl.when(tile == at)
            def _(at=at):
                at_each_place(SCHEDULE[1 + at])

        @pl.when(z == 0)
        def _():
            text_left(tile, False).wait_recv()

        @pl.when(z == last)
        def _():
            text_right(tile, False).wait_recv()

        attend(tile)
        send_attended(tile)

    at_each_place(SCHEDULE[-1])
    for mask in range(1, ranks):
        dest_copy(mask).wait_send()
    img.drain()
    qkv.drain()
    for k in range(mp_count):
        wout(k).drain()
    for tile in range(tiles):

        @pl.when((z >= first) & (z < last))
        def _():
            text_right(tile, False).wait_send()

        @pl.when(z > 0)
        def _():
            text_left(tile, False).wait_send()

        for part in range(mp_count):

            @pl.when(part != z)
            def _():
                att_copy(part, z, tile).wait_send()

    for block in range(mp_count):

        @pl.when((block <= z) & (z < last))
        def _():
            woutz_right(block).wait_send()

        @pl.when((block >= z) & (z > 0))
        def _():
            woutz_left(block).wait_send()

    for shard in range(shards):

        @pl.when((shard <= z) & (z < last))
        def _():
            imgz_right(shard).wait_send()

        @pl.when((shard >= z) & (z > 0))
        def _():
            imgz_left(shard).wait_send()

    @pl.loop(0, ranks)
    def _(source):
        out_copy(source).wait()


def fused_body(
    vit_features,
    patch_counts,
    text_counts,
    tile_dest,
    text_embeds,
    w_proj,
    b_proj,
    norm_gain,
    w_qkv,
    w_out,
):
    ranks = lax.axis_size("dp")
    mp_count = lax.axis_size("mp")
    tiles, local_rows, vision_width = vit_features.shape
    tile_size = local_rows * mp_count
    model_width = w_proj.shape[1]
    image_rows = tiles * local_rows
    shards = 3 * tile_size // 4 // local_rows
    images = vit_features.reshape(image_rows, vision_width)
    qkv_local = w_qkv.reshape(w_qkv.shape[1], -1)
    depth, qkv_width = qkv_local.shape
    out_depth = w_out.shape[1] * w_out.shape[2]
    out_width = w_out.shape[3]
    out_local = w_out.reshape(out_depth, out_width)

    half_size = HS // 2
    inverse = np.exp(
        -(2.0 * np.arange(half_size, dtype=np.float32) / HS) * math.log(rope_base)
    ).astype(np.float32)
    angles = np.arange(tile_size, dtype=np.float32)[:, None] * inverse[None, :]
    cosine, sine = np.cos(angles), np.sin(angles)
    cosine = jnp.asarray(np.concatenate([cosine, cosine], axis=1))
    sine = jnp.asarray(np.concatenate([-sine, sine], axis=1))

    orders = []
    for here in range(mp_count):
        order = [here]
        for distance in range(1, mp_count):
            nearer = distance if here < mp_count // 2 else -distance
            order += [at for at in (here - nearer, here + nearer) if 0 <= at < mp_count]
        orders.append(order)

    anywhere = pl.BlockSpec(memory_space=pl.ANY)
    smem = pl.BlockSpec(memory_space=pltpu.SMEM)
    half = jnp.bfloat16
    dma = pltpu.SemaphoreType.DMA
    return pl.pallas_call(
        functools.partial(fused_kernel, orders),
        in_specs=[smem, smem, smem] + [anywhere] * 9,
        out_specs=anywhere,
        out_shape=jax.ShapeDtypeStruct((tiles, local_rows, model_width), half),
        scratch_shapes=[
            pltpu.VMEM((1, model_width), jnp.float32),
            pltpu.VMEM((1, model_width), jnp.float32),
            pltpu.VMEM(cosine.shape, jnp.float32),
            pltpu.VMEM(sine.shape, jnp.float32),
            pltpu.VMEM((ranks, tiles, LANES), jnp.int32),
            pltpu.VMEM((ranks,) + images.shape, half),
            pltpu.VMEM((shards, tiles, local_rows, vision_width), half),
            pltpu.VMEM((3, tiles, local_rows, model_width), half),
            pltpu.VMEM((ranks * depth, qkv_width), half),
            pltpu.VMEM((mp_count, ranks, out_depth, out_width), half),
            pltpu.VMEM((vision_width, model_width), half),
            pltpu.VMEM((tile_size, model_width), half),
            pltpu.VMEM((tile_size, model_width), half),
            pltpu.VMEM((tile_size, qkv_width), jnp.float32),
            pltpu.VMEM((mp_count, tiles, local_rows, out_depth), half),
            pltpu.VMEM((mp_count, tiles, local_rows, out_depth), half),
            pltpu.VMEM((tiles, local_rows, model_width), half),
            pltpu.VMEM((image_rows, model_width), jnp.float32),
            dma((9,)),
            dma((ranks,)),
            dma((ranks,)),
            dma((PLANE_STEPS,)),
            dma((PLANE_STEPS,)),
            dma((PLANE_STEPS,)),
            dma((PLANE_STEPS,)),
            dma((mp_count * PLANE_STEPS,)),
            dma((mp_count * PLANE_STEPS,)),
            dma((2 * tiles,)),
            dma((2 * tiles,)),
            dma((2 * shards,)),
            dma((shards,)),
            dma((2 * mp_count,)),
            dma((mp_count,)),
            dma((mp_count * tiles,)),
            dma((mp_count * tiles,)),
            dma((ranks,)),
        ],
        compiler_params=pltpu.CompilerParams(
            vmem_limit_bytes=VMEM_BYTES, has_side_effects=True, collective_id=0
        ),
        name="fused",
    )(
        patch_counts,
        text_counts,
        tile_dest,
        images,
        text_embeds,
        w_proj,
        qkv_local,
        out_local,
        b_proj.reshape(1, -1),
        norm_gain.reshape(1, -1),
        cosine,
        sine,
    )


def body(*arrays):
    vit_features = arrays[0]
    local_rows = vit_features.shape[1]
    tile_size = local_rows * lax.axis_size("mp")
    outer_axes = (lax.axis_size("dp") // 2).bit_length() - 1
    if outer_axes == 2 and lax.axis_size("mp") == len(SCHEDULE[0]):
        return fused_body(*arrays)
    return general_body(*arrays)


def solution(mesh):
    in_specs = (
        P("dp", "mp", None),
        P("dp"),
        P("dp"),
        P("dp"),
        P("dp", "mp", None),
        P(),
        P(),
        P(),
        P(None, "dp", "mp", None),
        P(None, "mp", None, "dp"),
    )
    out_specs = P("dp", "mp", None)
    return jax.shard_map(body, mesh=mesh, in_specs=in_specs, out_specs=out_specs, check_vma=False)
```
